32 devices in a mesh: dp: 8 (over y, x, core), tp: 4 (over z).
Axes of the slice: x: 2, y: 2, z: 4, core: 2. Of those that a mesh axis runs over, the one named last changes fastest.
Arguments:
- tokens: bfloat16 [4096, 4096], P(('dp', 'tp')), may hold values from -6 to 6
- norm_gain: float32 [4096], replicated, may hold values from 0.1 to 1.9
- w_query: bfloat16 [4096, 4096], P(None, 'tp'), may hold values from -0.09375 to 0.09375
- w_key: bfloat16 [4096, 1024], P(None, 'tp'), may hold values from -2.34375 to 2.34375
- w_value: bfloat16 [4096, 1024], P(None, 'tp'), may hold values from -0.09375 to 0.09375
- w_output: bfloat16 [4096, 4096], P('tp'), may hold values from -0.09375 to 0.09375
- doc_lengths: int32 [32], replicated, may hold values from 1 to 512, as said below
- pack_index: int32 [4096], replicated, may hold values from 0 to 4095, as said below
Outputs:
- output: bfloat16 [4096, 4096], P(('dp', 'tp'))
The draws below stay inside these ranges and needn't reach their ends.
Inputs may be any that keep to these rules, and one draw needn't show every extreme that they name: `doc_lengths`: each run of 4 documents numbered g * 4 to g * 4 + 4 - 1 (the documents of group g) holds at most 1024 tokens together, and some group holds exactly 1024. No document is longer than 512 tokens, and one has exactly that many. `pack_index`: each packed position appears once. The 128 rows of one device hold at most 32 tokens of the documents of any one group; every device holds the same number of one group's tokens, up to one.
All inputs are finite; a program needn't handle non-finite values.
Results may differ from the reference program's by a relative error of at most 0.01.
Values may be sent and summed in bfloat16 or wider, within the bound.
A program may use at most 128 MiB of HBM per device.

```python
import jax
import jax.numpy as jnp
from jax import lax

D = 4096
HEADS = 32
KV_HEADS = 8
HEAD_DIM = 128
TOK_DEV = 128
GROUP_DOCS = 4
TOKENS = 4096
DOCS = 32
CAP = 1024
N_DP = 8
DEVICES = 32


def query_columns(key):
    return jax.random.truncated_normal(jax.random.fold_in(key, 11), -6.0, 6.0, (D, HEADS * HEAD_DIM), jnp.float32) * D ** (-0.5)


def draw_w_query(key, part):
    return query_columns(key).astype(jnp.bfloat16)


def draw_w_key(key, part):
    own_draw = jax.random.truncated_normal(jax.random.fold_in(key, 13), -6.0, 6.0, (D, KV_HEADS * HEAD_DIM), jnp.float32) * D ** (-0.5)
    return own_draw.astype(jnp.bfloat16)


def layout_plan(key):
    root_random_key = jax.random.fold_in(key, 29)
    complete_random_key, split_random_key, reward_random_key, jitter_random_key, permute_random_key, turning_random_key = jax.random.split(root_random_key, 6)
    full_group = jax.random.randint(complete_random_key, (), 0, N_DP).astype(jnp.int32)
    half_cap = CAP // 2
    cut_points = jnp.sort(jax.random.permutation(split_random_key, half_cap - 1)[:GROUP_DOCS - 2] + 1).astype(jnp.int32)
    fences = jnp.concatenate([jnp.zeros((1,), jnp.int32), cut_points, jnp.full((1,), half_cap, jnp.int32)])
    lesser_lengths = fences[1:] - fences[:-1]
    unrolled = jnp.concatenate([jnp.full((1,), half_cap, jnp.int32), lesser_lengths])
    turning = jax.random.randint(turning_random_key, (), 0, GROUP_DOCS).astype(jnp.int32)
    full_lengths = jnp.roll(unrolled, turning).astype(jnp.int32)
    remaining_documents = (N_DP - 1) * GROUP_DOCS
    spare_capacity = CAP // GROUP_DOCS - 1
    extra_total = TOKENS - CAP - remaining_documents
    extra_reward = jax.random.randint(reward_random_key, (remaining_documents, 1), 0, 4).astype(jnp.int32)
    random_jitter = jax.random.randint(jitter_random_key, (remaining_documents, spare_capacity), 0, 1024).astype(jnp.int32)
    score_values = (extra_reward * 300 + random_jitter) * (remaining_documents * spare_capacity) + jnp.arange(remaining_documents * spare_capacity, dtype=jnp.int32).reshape(remaining_documents, spare_capacity)
    chosen = lax.top_k(score_values.reshape(-1), extra_total)[1].astype(jnp.int32)
    other_lengths = 1 + jax.ops.segment_sum(jnp.ones_like(chosen), chosen // spare_capacity, remaining_documents).astype(jnp.int32)
    slots = jnp.arange(DOCS, dtype=jnp.int32)
    slot_group = slots // GROUP_DOCS
    other_place = jnp.clip(slots - GROUP_DOCS * (slot_group > full_group).astype(jnp.int32), 0, remaining_documents - 1)
    lengths = jnp.where(slot_group == full_group, full_lengths[slots % GROUP_DOCS], other_lengths[other_place]).astype(jnp.int32)
    doc_ends = jnp.cumsum(lengths).astype(jnp.int32)
    doc_starts = doc_ends - lengths
    dealing = jnp.arange(TOKENS, dtype=jnp.int32)
    inside = ((dealing[:, None] >= doc_starts[None, :]) & (dealing[:, None] < doc_ends[None, :])).astype(jnp.int32)
    which_doc = jnp.sum(inside * jnp.arange(DOCS, dtype=jnp.int32)[None, :], axis=1)
    offset = dealing - jnp.sum(inside * doc_starts[None, :], axis=1)
    packed = doc_starts[which_doc] + offset
    dealt = packed.reshape(TOK_DEV, DEVICES).T
    shuffle = jnp.argsort(jax.random.randint(permute_random_key, (DEVICES, TOK_DEV), 0, 1 << 20).astype(jnp.int32) * TOK_DEV + jnp.arange(TOK_DEV, dtype=jnp.int32)[None, :], axis=1)
    placed = jnp.take_along_axis(dealt, shuffle, axis=1).reshape(TOKENS).astype(jnp.int32)
    return (lengths, placed)


def draw_doc_lengths(key, part):
    return layout_plan(key)[0]


def draw_pack_index(key, part):
    return layout_plan(key)[1]


def shard_levels(key, shape, pieces, low, largest):
    def one(axis_at, shards_of):
        heights = jax.random.uniform(jax.random.fold_in(jax.random.fold_in(key, 6), axis_at), (shards_of,), jnp.float32, low / len(pieces), largest / len(pieces))
        return jnp.repeat(jnp.exp(heights), shape[axis_at] // shards_of).reshape((-1,) + (1,) * (len(shape) - axis_at - 1))

    loudness = one(*pieces[0])
    for cut in pieces[1:]:
        loudness = loudness * one(*cut)
    return loudness


def bell_draw(rng, dims, width, bound, cuts=(), held_as=jnp.bfloat16):
    drawn = jax.random.normal(rng, dims, jnp.float32) * width
    if len(cuts) > 0:
        drawn = shard_levels(rng, dims, cuts, -0.22, 0.18) * drawn
    return jnp.clip(drawn, min=-bound, max=bound).astype(held_as)


def setup_inputs(seed: int = 0) -> dict:
    keys = jax.random.split(jax.random.key(seed), 9)
    return {
        "tokens": bell_draw(keys[0], (TOKENS, D), 1.0, 6.0, ((0, 32),)),
        "norm_gain": jnp.clip(1.0 + 0.18 * jax.random.normal(keys[1], (D,), jnp.float32), 0.1, 1.9),
        "w_query": draw_w_query(jax.random.fold_in(keys[8], 71), 0),
        "w_key": draw_w_key(jax.random.fold_in(keys[8], 71), 0),
        "w_value": bell_draw(keys[4], (D, KV_HEADS * HEAD_DIM), D ** -0.5, 0.09375, ((1, 4),)),
        "w_output": bell_draw(keys[5], (HEADS * HEAD_DIM, D), (HEADS * HEAD_DIM) ** -0.5, 0.09375, ((0, 4),)),
        "doc_lengths": draw_doc_lengths(jax.random.fold_in(keys[8], 71), 0),
        "pack_index": draw_pack_index(jax.random.fold_in(keys[8], 71), 0),
    }


rope_base = 500000.0
norm_eps = 1e-05
score_floor = -1e+30

def row_facts(pack_index, doc_lengths):
    doc_ends = jnp.cumsum(doc_lengths).astype(jnp.int32)
    doc_starts = doc_ends - doc_lengths
    inside = ((pack_index[:, None] >= doc_starts[None, :]) & (pack_index[:, None] < doc_ends[None, :])).astype(jnp.int32)
    doc_index = lax.optimization_barrier(jnp.sum(inside * jnp.arange(doc_lengths.shape[0], dtype=jnp.int32)[None, :], axis=1))
    position = pack_index - lax.optimization_barrier(jnp.sum(inside * doc_starts[None, :], axis=1))
    owner_group = (doc_index // GROUP_DOCS).astype(jnp.int32)
    return (doc_index, position, owner_group)

def rotate(projected, position, head_count):
    row_count = projected.shape[0]
    half_dim = HEAD_DIM // 2
    spread = projected.reshape(row_count, head_count, HEAD_DIM)
    frequency = rope_base ** (-2.0 * jnp.arange(half_dim, dtype=jnp.float32) / HEAD_DIM)
    angles = position.astype(jnp.float32)[:, None] * frequency[None, :]
    cosine = jnp.cos(angles)[:, None, :]
    sine = jnp.sin(angles)[:, None, :]
    lower_part = spread[:, :, :half_dim]
    upper_part = spread[:, :, half_dim:]
    turned = jnp.concatenate([lower_part * cosine - upper_part * sine, upper_part * cosine + lower_part * sine], axis=2)
    return turned.reshape(row_count, head_count * HEAD_DIM)

def attend_exact(query, key_rows, value_rows, segment, places):
    slot_total = query.shape[0]
    group_size = HEADS // KV_HEADS
    query_heads = query.astype(jnp.float32).reshape(slot_total, KV_HEADS, group_size, HEAD_DIM)
    key_heads = key_rows.astype(jnp.float32).reshape(slot_total, KV_HEADS, HEAD_DIM)
    value_heads = value_rows.astype(jnp.float32).reshape(slot_total, KV_HEADS, HEAD_DIM)
    score_values = jnp.einsum('qkgd,skd->kgqs', query_heads, key_heads, precision=lax.Precision.HIGHEST) * HEAD_DIM ** (-0.5)
    allowed = (segment[:, None] == segment[None, :]) & (places[None, :] <= places[:, None])
    score_values = jnp.where(allowed[None, None], score_values, score_floor)
    row_peak = lax.optimization_barrier(jnp.max(score_values, axis=-1, keepdims=True))
    weights = jnp.exp(score_values - row_peak)
    weights = (weights / lax.optimization_barrier(jnp.sum(weights, axis=-1, keepdims=True))).astype(jnp.bfloat16)
    mixed_values = jnp.einsum('kgqs,skd->qkgd', weights.astype(jnp.float32), value_heads, precision=lax.Precision.HIGHEST)
    return mixed_values.astype(jnp.bfloat16).reshape(slot_total, HEADS * HEAD_DIM)

def reference(tokens, norm_gain, w_query, w_key, w_value, w_output, doc_lengths, pack_index):
    doc_index, position, owner_group = row_facts(pack_index, doc_lengths)
    residual = tokens.astype(jnp.float32)
    normed = (residual * lax.rsqrt(lax.optimization_barrier(jnp.mean(residual * residual, axis=1, keepdims=True)) + norm_eps) * norm_gain).astype(jnp.bfloat16)
    query = rotate(jnp.dot(normed, w_query, preferred_element_type=jnp.float32), position, HEADS).astype(jnp.bfloat16)
    key_rows = rotate(jnp.dot(normed, w_key, preferred_element_type=jnp.float32), position, KV_HEADS).astype(jnp.bfloat16)
    value_rows = jnp.dot(normed, w_value, preferred_element_type=jnp.float32).astype(jnp.bfloat16)
    ranked = jnp.argsort(owner_group * TOKENS + jnp.arange(TOKENS, dtype=jnp.int32)).astype(jnp.int32)
    counts = jax.ops.segment_sum(jnp.ones((TOKENS,), jnp.int32), owner_group, N_DP).astype(jnp.int32)
    firsts = (jnp.cumsum(counts) - counts).astype(jnp.int32)
    padded = jnp.concatenate([ranked, jnp.zeros((CAP,), jnp.int32)])
    slot_ids = jnp.arange(CAP, dtype=jnp.int32)

    def one_group(gathered, group_id):
        chosen = lax.dynamic_slice_in_dim(padded, firsts[group_id], CAP)
        occupied = slot_ids < counts[group_id]
        segment = jnp.where(occupied, doc_index[chosen], -1 - slot_ids)
        places = jnp.where(occupied, position[chosen], 0)
        context = attend_exact(query[chosen], key_rows[chosen], value_rows[chosen], segment, places)
        target = jnp.where(occupied, chosen, TOKENS)
        return (gathered.at[target].set(context, mode='drop'), None)
    gathered, _ = lax.scan(one_group, jnp.zeros((TOKENS, HEADS * HEAD_DIM), jnp.bfloat16), jnp.arange(N_DP, dtype=jnp.int32))
    attended = jnp.dot(gathered, w_output, preferred_element_type=jnp.float32)
    return (residual + attended).astype(jnp.bfloat16)
```

```python
import functools

import jax
import jax.numpy as jnp
from jax import lax
from jax.experimental import pallas as pl
from jax.experimental.pallas import tpu as pltpu
from jax.sharding import PartitionSpec as P

HEAD_DIM = 128
GROUP_DOCS = 4
LOG2E = 1.4426950408889634

rope_base = 500000.0
norm_eps = 1e-05
score_floor = -1e30
VMEM_BYTES = 60 * 1024 * 1024
MESH = pl.DeviceIdType.MESH
VMEM_SPEC = pl.BlockSpec(memory_space=pltpu.VMEM)


def remote(src, dst, send_sem, recv_sem, where):
    return pltpu.make_async_remote_copy(
        src_ref=src,
        dst_ref=dst,
        send_sem=send_sem,
        recv_sem=recv_sem,
        device_id=where,
        device_id_type=MESH,
    )


def greet(peers):
    barrier = pltpu.get_barrier_semaphore()
    for where in peers:
        pl.semaphore_signal(barrier, inc=1, device_id=where, device_id_type=MESH)
    pl.semaphore_wait(barrier, len(peers))


def project_kernel(
    exchange, x_ref, wq_ref, wk_ref, wv_ref, cos_ref, sin_ref, sort_ref,
    q_out, kv_out, gathered, mixed_q, mixed_kv, send_sem, recv_sem, kv_send, kv_recv,
):
    tok = x_ref.shape[0]
    half = tok // 2
    dp = lax.axis_index("dp")
    me = lax.axis_index("tp")
    right, left = lax.rem(me + 1, 4), lax.rem(me + 3, 4)
    far = lax.rem(me + 2, 4)
    go_right, go_left = (dp, right), (dp, left)
    core = lax.rem(dp, 2)
    x_at = lax.rem(dp // 2, 2)
    y_at = dp // 4
    mate = dp + 1 - 2 * core
    x_near = dp + 2 - 4 * x_at
    y_near = dp + 4 - 8 * y_at
    peers = [go_right, go_left]
    if exchange:
        peers += [(mate, me), (x_near, me), (y_near, me)]
    greet(peers)

    def rows(owner, start=0, size=tok):
        return pl.ds(pl.multiple_of(owner * tok + start, size), size)

    own_right = remote(x_ref, gathered.at[rows(me)], send_sem.at[0], recv_sem.at[0], go_right)
    own_left = remote(x_ref, gathered.at[rows(me)], send_sem.at[1], recv_sem.at[1], go_left)
    own_right.start()
    own_left.start()

    def project(owner, block):
        cosine = cos_ref[rows(owner), :]
        sine = sin_ref[rows(owner), :]

        def turn(tile):
            heads = []
            for h in range(tile.shape[1] // HEAD_DIM):
                head = tile[:, h * HEAD_DIM : (h + 1) * HEAD_DIM]
                heads.append(head * cosine + pltpu.roll(head, HEAD_DIM // 2, 1) * sine)
            return jnp.concatenate(heads, axis=1).astype(jnp.bfloat16)

        kv_width = wk_ref.shape[1]
        keys = jnp.dot(block[...], wk_ref[...], preferred_element_type=jnp.float32)
        mixed_kv[rows(owner), pl.ds(0, kv_width)] = turn(keys)
        values = jnp.dot(block[...], wv_ref[...], preferred_element_type=jnp.float32)
        mixed_kv[rows(owner), pl.ds(kv_width, kv_width)] = values.astype(jnp.bfloat16)

        def step(i, _):
            columns = pl.ds(pl.multiple_of(i * 256, 256), 256)
            tile = jnp.dot(block[...], wq_ref[:, columns], preferred_element_type=jnp.float32)
            mixed_q[rows(owner), columns] = turn(tile)
            return 0

        lax.fori_loop(0, wq_ref.shape[1] // 256, step, 0)

    project(me, x_ref)
    own_right.wait_recv()
    top = gathered.at[rows(left, 0, half)]
    pass_right = remote(top, top, send_sem.at[2], recv_sem.at[2], go_right)
    pass_right.start()
    own_left.wait_recv()
    low = gathered.at[rows(right, half, half)]
    pass_left = remote(low, low, send_sem.at[3], recv_sem.at[3], go_left)
    pass_left.start()
    project(left, gathered.at[rows(left)])
    project(right, gathered.at[rows(right)])
    pass_right.wait_recv()
    pass_left.wait_recv()
    project(far, gathered.at[rows(far)])

    own = kv_out.at[dp] if exchange else kv_out.at[0]
    own[...] = jnp.dot(
        sort_ref[...], mixed_kv[...], preferred_element_type=jnp.float32
    ).astype(jnp.bfloat16)
    started = [own_right, own_left, pass_right, pass_left]
    if exchange:
        span = kv_out.shape[1]
        upper, lower = pl.ds(0, span // 2), pl.ds(span // 2, span // 2)
        cross = x_near + y_near - dp

        def put(ref, i, where):
            copy = remote(ref, ref, kv_send.at[i], kv_recv.at[i], (where, me))
            copy.start()
            return copy

        to_x = put(kv_out.at[dp], 0, x_near)
        to_y = put(kv_out.at[dp], 1, y_near)
        to_mate = put(kv_out.at[dp], 2, mate)

    def sort_step(i, _):
        columns = pl.ds(pl.multiple_of(i * 256, 256), 256)
        q_out[:, columns] = jnp.dot(
            sort_ref[...], mixed_q[:, columns], preferred_element_type=jnp.float32
        ).astype(jnp.bfloat16)
        return 0

    lax.fori_loop(0, wq_ref.shape[1] // 256, sort_step, 0)

    if exchange:
        to_x.wait_recv()
        x_over = put(kv_out.at[x_near, upper], 3, y_near)
        x_mate = put(kv_out.at[x_near], 4, mate)
        to_y.wait_recv()
        y_over = put(kv_out.at[y_near, lower], 5, x_near)
        y_mate = put(kv_out.at[y_near], 6, mate)
        x_over.wait_recv()
        up_mate = put(kv_out.at[cross, upper], 7, mate)
        y_over.wait_recv()
        low_mate = put(kv_out.at[cross, lower], 8, mate)
        for copy in (to_mate, x_mate, y_mate, up_mate, low_mate):
            copy.wait_recv()
        started += [to_x, to_y, to_mate, x_over, x_mate, y_over, y_mate, up_mate, low_mate]
    for copy in started:
        copy.wait_send()


def project(normed, w_query, w_key, w_value, cosine, sine, sort, exchange, group_count):
    tok, width = normed.shape
    span = 4 * tok
    q_width, kv_width = w_query.shape[1], w_key.shape[1]
    slots = group_count if exchange else 1
    return pl.pallas_call(
        functools.partial(project_kernel, exchange),
        out_shape=(
            jax.ShapeDtypeStruct((span, q_width), jnp.bfloat16),
            jax.ShapeDtypeStruct((slots, span, 2 * kv_width), jnp.bfloat16),
        ),
        in_specs=[VMEM_SPEC] * 7,
        out_specs=(VMEM_SPEC, VMEM_SPEC),
        scratch_shapes=[
            pltpu.VMEM((span, width), jnp.bfloat16),
            pltpu.VMEM((span, q_width), jnp.bfloat16),
            pltpu.VMEM((span, 2 * kv_width), jnp.bfloat16),
            pltpu.SemaphoreType.DMA((4,)),
            pltpu.SemaphoreType.DMA((4,)),
            pltpu.SemaphoreType.DMA((9,)),
            pltpu.SemaphoreType.DMA((9,)),
        ],
        compiler_params=pltpu.CompilerParams(
            collective_id=0, has_side_effects=True, vmem_limit_bytes=VMEM_BYTES
        ),
        name="project",
    )(normed, w_query, w_key, w_value, cosine, sine, sort)


def attend_kernel(
    key_rows, q_rows, bounds_ref, q_ref, kv_ref, key_place_ref, q_place_ref, q_start_ref, back_ref,
    out_ref, context,
):
    sources = kv_ref.shape[0]
    kv_count = kv_ref.shape[2] // (2 * HEAD_DIM)
    group = q_ref.shape[1] // HEAD_DIM // kv_count
    chunk = sources * key_rows
    scale = HEAD_DIM ** (-0.5) * LOG2E
    stack = group * q_rows

    def tile_step(t, _):
        at = pl.ds(pl.multiple_of(t * q_rows, q_rows), q_rows)
        place = q_place_ref[at, :]
        start = q_start_ref[at, :]
        queries = []
        for h in range(kv_count):
            queries.append(
                jnp.concatenate(
                    [
                        q_ref[at, (h * group + j) * HEAD_DIM : (h * group + j + 1) * HEAD_DIM]
                        for j in range(group)
                    ],
                    axis=0,
                )
            )

        def chunk_step(b, carry):
            places = key_place_ref[b]
            bias = jnp.where(
                (places >= start) & (places <= place), jnp.float32(0), jnp.float32(score_floor)
            )
            bias = jnp.concatenate([bias] * group, axis=0)
            rows = pl.ds(pl.multiple_of(b * key_rows, key_rows), key_rows)
            after = []
            for h in range(kv_count):
                peak, total, mixed = carry[h]
                keys = kv_ref[:, rows, h * HEAD_DIM : (h + 1) * HEAD_DIM].reshape(chunk, HEAD_DIM)
                low = (kv_count + h) * HEAD_DIM
                values = kv_ref[:, rows, low : low + HEAD_DIM].reshape(chunk, HEAD_DIM)
                scores = (
                    lax.dot_general(
                        queries[h], keys, (((1,), (1,)), ((), ())),
                        preferred_element_type=jnp.float32,
                    )
                    * scale
                    + bias
                )
                new_peak = jnp.maximum(peak, jnp.max(scores, axis=1, keepdims=True))
                weights = jnp.exp2(scores - new_peak)
                fade = jnp.exp2(peak - new_peak)
                total = total * fade + jnp.sum(weights, axis=1, keepdims=True)
                mixed = mixed * fade + jnp.dot(
                    weights.astype(jnp.bfloat16), values, preferred_element_type=jnp.float32
                )
                after.append((new_peak, total, mixed))
            return tuple(after)

        first = tuple(
            (
                jnp.full((stack, 1), score_floor, jnp.float32),
                jnp.zeros((stack, 1), jnp.float32),
                jnp.zeros((stack, HEAD_DIM), jnp.float32),
            )
            for _ in range(kv_count)
        )
        last = lax.fori_loop(bounds_ref[0, t], bounds_ref[1, t], chunk_step, first)
        for h in range(kv_count):
            _, total, mixed = last[h]
            done = (mixed / total).astype(jnp.bfloat16)
            for j in range(group):
                head = (h * group + j) * HEAD_DIM
                context[at, head : head + HEAD_DIM] = done[j * q_rows : (j + 1) * q_rows]
        return 0

    lax.fori_loop(0, q_ref.shape[0] // q_rows, tile_step, 0)

    def back_step(i, _):
        columns = pl.ds(pl.multiple_of(i * 256, 256), 256)
        out_ref[:, columns] = jnp.dot(
            back_ref[...], context[:, columns], preferred_element_type=jnp.float32
        ).astype(jnp.bfloat16)
        return 0

    lax.fori_loop(0, q_ref.shape[1] // 256, back_step, 0)


def attend(bounds, query, kv_all, key_place, q_place, q_start, back, key_rows, q_rows):
    return pl.pallas_call(
        functools.partial(attend_kernel, key_rows, q_rows),
        out_shape=jax.ShapeDtypeStruct(query.shape, jnp.bfloat16),
        in_specs=[pl.BlockSpec(memory_space=pltpu.SMEM)] + [VMEM_SPEC] * 6,
        out_specs=VMEM_SPEC,
        scratch_shapes=[pltpu.VMEM(query.shape, jnp.bfloat16)],
        compiler_params=pltpu.CompilerParams(vmem_limit_bytes=VMEM_BYTES),
        name="attend",
    )(bounds, query, kv_all, key_place, q_place, q_start, back)


def output_kernel(
    context_ref, w_ref, tokens_ref, out_ref,
    far_out, right_out, left_out, relay, from_left, from_right, send_sem, recv_sem,
):
    tok, width = tokens_ref.shape
    half = width // 2
    dp = lax.axis_index("dp")
    me = lax.axis_index("tp")
    right, left = lax.rem(me + 1, 4), lax.rem(me + 3, 4)
    far = lax.rem(me + 2, 4)
    go_right, go_left = (dp, right), (dp, left)
    greet([go_right, go_left])
    columns = (pl.ds(0, half), pl.ds(half, half))
    tile = 256

    def fill(owner, dst, side, more=None):
        rows = pl.ds(pl.multiple_of(owner * tok, tok), tok)

        def step(i, _):
            at = pl.ds(pl.multiple_of(side * half + i * tile, tile), tile)
            term = jnp.dot(context_ref[rows, :], w_ref[:, at], preferred_element_type=jnp.float32)
            if more is not None:
                part = pl.ds(pl.multiple_of(i * tile, tile), tile)
                term = term + more[:, part].astype(jnp.float32)
            at_half = pl.ds(pl.multiple_of(i * tile, tile), tile)
            dst[side, :, at_half] = term.astype(jnp.bfloat16)
            return 0

        lax.fori_loop(0, half // tile, step, 0)

    def put(src, dst, i, where):
        copy = remote(src, dst, send_sem.at[i], recv_sem.at[i], where)
        copy.start()
        return copy

    fill(far, far_out, 0)
    far_right = put(far_out.at[0], relay.at[0], 0, go_right)
    fill(far, far_out, 1)
    far_left = put(far_out.at[1], relay.at[1], 1, go_left)
    fill(right, right_out, 1)
    near_right = put(right_out.at[1], from_left.at[1], 2, go_right)
    fill(left, left_out, 0)
    near_left = put(left_out.at[0], from_right.at[0], 3, go_left)
    far_right.wait_recv()
    fill(right, right_out, 0, relay.at[0])
    sum_right = put(right_out.at[0], from_left.at[0], 4, go_right)
    far_left.wait_recv()
    fill(left, left_out, 1, relay.at[1])
    sum_left = put(left_out.at[1], from_right.at[1], 5, go_left)
    near_right.wait_recv()
    near_left.wait_recv()

    rows = pl.ds(pl.multiple_of(me * tok, tok), tok)
    sums = (sum_right, sum_left)
    for copy in sums:
        copy.wait_recv()
    for side in range(2):

        def last_step(i, _):
            at = pl.ds(pl.multiple_of(side * half + i * tile, tile), tile)
            part = pl.ds(pl.multiple_of(i * tile, tile), tile)
            term = jnp.dot(context_ref[rows, :], w_ref[:, at], preferred_element_type=jnp.float32)
            term = term + from_left[side, :, part].astype(jnp.float32)
            term = term + from_right[side, :, part].astype(jnp.float32)
            out_ref[:, at] = (term + tokens_ref[:, at].astype(jnp.float32)).astype(jnp.bfloat16)
            return 0

        lax.fori_loop(0, half // tile, last_step, 0)
    for copy in (far_right, far_left, near_right, near_left, sum_right, sum_left):
        copy.wait_send()


def project_out(context, w_output, tokens):
    tok, width = tokens.shape
    pair = pltpu.VMEM((2, tok, width // 2), jnp.bfloat16)
    return pl.pallas_call(
        output_kernel,
        out_shape=jax.ShapeDtypeStruct(tokens.shape, jnp.bfloat16),
        in_specs=[VMEM_SPEC] * 3,
        out_specs=VMEM_SPEC,
        scratch_shapes=[pair] * 6
        + [pltpu.SemaphoreType.DMA((6,)), pltpu.SemaphoreType.DMA((6,))],
        compiler_params=pltpu.CompilerParams(
            collective_id=1, has_side_effects=True, vmem_limit_bytes=VMEM_BYTES
        ),
        name="project_out",
    )(context, w_output, tokens)


def body(tokens, norm_gain, w_query, w_key, w_value, w_output, doc_lengths, pack_index):
    group_count = lax.axis_size("dp")
    tp_count = lax.axis_size("tp")
    tok_dev = tokens.shape[0]
    span = tp_count * tok_dev
    my_group = lax.axis_index("dp")
    exchange = group_count == 8
    q_rows = 64
    key_rows = max(16, 512 // group_count)
    key_chunks = span // key_rows

    packs = pack_index.reshape(group_count, span)
    order = jnp.arange(span, dtype=jnp.int32)
    rank = jnp.sum((packs[:, None, :] < packs[:, :, None]).astype(jnp.int32), axis=2)
    sorted_packs = jnp.sum(
        jnp.where(rank[:, None, :] == order[None, :, None], packs[:, None, :], 0), axis=2
    )
    key_place = (
        sorted_packs.reshape(group_count, key_chunks, key_rows)
        .transpose(1, 0, 2)
        .reshape(key_chunks, 1, group_count * key_rows)
    )
    chunk_low = jnp.min(key_place, axis=(1, 2))
    chunk_high = jnp.max(key_place, axis=(1, 2))

    doc_ends = jnp.cumsum(doc_lengths)
    doc_starts = doc_ends - doc_lengths

    def start_of(place):
        inside = (place[:, None] >= doc_starts[None, :]) & (place[:, None] < doc_ends[None, :])
        return jnp.sum(jnp.where(inside, doc_starts[None, :], 0), axis=1)

    my_pack = lax.dynamic_index_in_dim(packs, my_group, 0, keepdims=False)
    my_rank = lax.dynamic_index_in_dim(rank, my_group, 0, keepdims=False)
    my_sorted = lax.dynamic_index_in_dim(sorted_packs, my_group, 0, keepdims=False)
    sort = (my_rank[None, :] == order[:, None]).astype(jnp.bfloat16)
    back = (my_rank[:, None] == order[None, :]).astype(jnp.bfloat16)
    my_start = start_of(my_sorted)
    tile_low = my_start.reshape(-1, q_rows)[:, 0]
    tile_high = my_sorted.reshape(-1, q_rows)[:, -1]
    bounds = jnp.stack(
        [
            jnp.sum((chunk_high[None, :] < tile_low[:, None]).astype(jnp.int32), axis=1),
            jnp.sum((chunk_low[None, :] <= tile_high[:, None]).astype(jnp.int32), axis=1),
        ]
    )

    position = my_pack - start_of(my_pack)
    half_dim = HEAD_DIM // 2
    frequency = rope_base ** (-2.0 * jnp.arange(half_dim, dtype=jnp.float32) / HEAD_DIM)
    angles = position.astype(jnp.float32)[:, None] * frequency[None, :]
    cos_half, sin_half = jnp.cos(angles), jnp.sin(angles)
    cosine = jnp.concatenate([cos_half, cos_half], axis=1)
    sine = jnp.concatenate([-sin_half, sin_half], axis=1)

    residual = tokens.astype(jnp.float32)
    normed = (
        residual
        * lax.rsqrt(jnp.mean(residual * residual, axis=1, keepdims=True) + norm_eps)
        * norm_gain
    ).astype(jnp.bfloat16)
    query, kv = project(
        normed, w_query, w_key, w_value, cosine, sine, sort, exchange, group_count
    )
    if not exchange:
        kv = lax.all_gather(kv[0], "dp", axis=0)
    context = attend(
        bounds, query, kv, key_place, my_sorted[:, None], my_start[:, None], back, key_rows, q_rows
    )
    return project_out(context, w_output, tokens)


def solution(mesh):
    placed = (
        P(("dp", "tp"), None),
        P(),
        P(None, "tp"),
        P(None, "tp"),
        P(None, "tp"),
        P("tp", None),
        P(),
        P(),
    )
    return jax.shard_map(
        body, mesh=mesh, in_specs=placed, out_specs=P(("dp", "tp"), None), check_vma=False
    )
```

```python
import functools

import jax
import jax.numpy as jnp
from jax import lax
from jax.experimental import pallas as pl
from jax.experimental.pallas import tpu as pltpu
from jax.sharding import PartitionSpec as P

HEAD_DIM = 128
GROUP_DOCS = 4
LOG2E = 1.4426950408889634

rope_base = 500000.0
norm_eps = 1e-05
score_floor = -1e30
VMEM_BYTES = 60 * 1024 * 1024
MESH = pl.DeviceIdType.MESH
VMEM_SPEC = pl.BlockSpec(memory_space=pltpu.VMEM)


def remote(src, dst, send_sem, recv_sem, where):
    return pltpu.make_async_remote_copy(
        src_ref=src,
        dst_ref=dst,
        send_sem=send_sem,
        recv_sem=recv_sem,
        device_id=where,
        device_id_type=MESH,
    )


def greet(peers):
    barrier = pltpu.get_barrier_semaphore()
    for where in peers:
        pl.semaphore_signal(barrier, inc=1, device_id=where, device_id_type=MESH)
    pl.semaphore_wait(barrier, len(peers))


def project_kernel(
    exchange, x_ref, wq_hbm, wk_hbm, wv_hbm, cos_ref, sin_ref,
    q_out, kv_out, gathered, wq_ref, wk_ref, wv_ref,
    own_sem, send_sem, recv_sem, load_sem, kv_send, kv_recv,
):
    tok = x_ref.shape[0]
    dp = lax.axis_index("dp")
    me = lax.axis_index("tp")
    last = 3
    right, left = lax.rem(me + 1, 4), lax.rem(me + 3, 4)
    core = lax.rem(dp, 2)
    x_at = lax.rem(dp // 2, 2)
    y_at = dp // 4
    mate = dp + 1 - 2 * core
    x_near = dp + 2 - 4 * x_at
    y_near = dp + 4 - 8 * y_at
    cross = x_near + y_near - dp
    loads = [
        pltpu.make_async_copy(wk_hbm, wk_ref, load_sem.at[0]),
        pltpu.make_async_copy(wv_hbm, wv_ref, load_sem.at[1]),
        pltpu.make_async_copy(wq_hbm, wq_ref, load_sem.at[2]),
    ]
    for load in loads:
        load.start()
    peers = [(dp, right), (dp, left)]
    if exchange:
        peers += [(mate, me), (x_near, me), (y_near, me)]
    greet(peers)

    def rows(owner, start=0, size=tok):
        return pl.ds(pl.multiple_of(owner * tok + start, size), size)

    own_right = remote(x_ref, gathered.at[rows(me)], own_sem.at[0], recv_sem.at[me], (dp, right))
    own_left = remote(x_ref, gathered.at[rows(me)], own_sem.at[1], recv_sem.at[me], (dp, left))

    @pl.when(me < last)
    def _():
        own_right.start()

    @pl.when(me > 0)
    def _():
        own_left.start()

    order = ((0, 1, 2, 3), (1, 0, 2, 3), (2, 1, 3, 0), (3, 2, 1, 0))

    def owner_at(k):
        code = sum(order[m][k] << (2 * m) for m in range(4))
        return lax.rem(lax.shift_right_logical(jnp.int32(code), 2 * me), 4)

    def passing(owner, where):
        block = gathered.at[rows(owner)]
        return remote(block, block, send_sem.at[owner], recv_sem.at[owner], (dp, where))

    def receive(k):
        owner = owner_at(k)
        passing(owner, right).wait_recv()

        @pl.when((owner < me) & (me < last))
        def _():
            passing(owner, right).start()

        @pl.when((owner > me) & (me > 0))
        def _():
            passing(owner, left).start()

    own_slot = dp if exchange else 0
    kv_width = wk_ref.shape[1]

    def turn(owner, tile):
        cosine = cos_ref[rows(owner), :]
        sine = sin_ref[rows(owner), :]
        heads = []
        for h in range(tile.shape[1] // HEAD_DIM):
            head = tile[:, h * HEAD_DIM : (h + 1) * HEAD_DIM]
            heads.append(head * cosine + pltpu.roll(head, HEAD_DIM // 2, 1) * sine)
        return jnp.concatenate(heads, axis=1).astype(jnp.bfloat16)

    def project_kv(owner, block):
        keys = jnp.dot(block[...], wk_ref[...], preferred_element_type=jnp.float32)
        kv_out[own_slot, rows(owner), pl.ds(0, kv_width)] = turn(owner, keys)
        values = jnp.dot(block[...], wv_ref[...], preferred_element_type=jnp.float32)
        kv_out[own_slot, rows(owner), pl.ds(kv_width, kv_width)] = values.astype(jnp.bfloat16)

    def project_q(owner, block):
        def step(i, _):
            columns = pl.ds(pl.multiple_of(i * 256, 256), 256)
            tile = jnp.dot(block[...], wq_ref[:, columns], preferred_element_type=jnp.float32)
            q_out[rows(owner), columns] = turn(owner, tile)
            return 0

        lax.fori_loop(0, wq_ref.shape[1] // 256, step, 0)

    half = tok // 2
    started = []

    def put(ref, k, i, where):
        copy = remote(ref, ref, kv_send.at[k, i], kv_recv.at[k, i], (where, me))
        copy.start()
        started.append(copy)
        return copy

    def first_sends(k):
        block = kv_out.at[dp, rows(owner_at(k))]
        return put(block, k, 0, x_near), put(block, k, 1, y_near), put(block, k, 2, mate)

    def second_sends(k, sent):
        owner = owner_at(k)
        to_x, to_y, to_mate = sent
        to_x.wait_recv()
        x_over = put(kv_out.at[x_near, rows(owner, 0, half)], k, 3, y_near)
        x_mate = put(kv_out.at[x_near, rows(owner)], k, 4, mate)
        to_y.wait_recv()
        y_over = put(kv_out.at[y_near, rows(owner, half, half)], k, 5, x_near)
        y_mate = put(kv_out.at[y_near, rows(owner)], k, 6, mate)
        return owner, (x_over, y_over), (to_mate, x_mate, y_mate)

    def third_sends(k, sent):
        owner, (x_over, y_over), others = sent
        x_over.wait_recv()
        up_mate = put(kv_out.at[cross, rows(owner, 0, half)], k, 7, mate)
        y_over.wait_recv()
        low_mate = put(kv_out.at[cross, rows(owner, half, half)], k, 8, mate)
        return others + (up_mate, low_mate)

    ends = []
    for load in loads:
        load.wait()
    project_kv(me, x_ref)
    if exchange:
        sent0 = first_sends(0)
    project_q(me, x_ref)
    if exchange:
        sent0 = second_sends(0, sent0)
    receive(1)
    receive(2)
    if exchange:
        ends += third_sends(0, sent0)
    waiting = []
    for k in (1, 2, 3):
        owner = owner_at(k)
        if k == 3:
            receive(3)
        project_kv(owner, gathered.at[rows(owner)])
        if exchange:
            sent = first_sends(k)
            for j, old in waiting:
                ends += third_sends(j, old)
            waiting = []
        if k == 3 and exchange:
            sent = second_sends(k, sent)
        project_q(owner, gathered.at[rows(owner)])
        if exchange:
            if k < 3:
                sent = second_sends(k, sent)
            waiting = [(k, sent)]
    for j, old in waiting:
        ends += third_sends(j, old)
    for copy in ends:
        copy.wait_recv()
    for copy in started:
        copy.wait_send()

    @pl.when(me < last)
    def _():
        own_right.wait_send()

    @pl.when(me > 0)
    def _():
        own_left.wait_send()

    for k in (1, 2, 3):
        owner = owner_at(k)

        @pl.when(((owner < me) & (me < last)) | ((owner > me) & (me > 0)))
        def _():
            passing(owner, right).wait_send()


def project(normed, w_query, w_key, w_value, cosine, sine, exchange, group_count):
    tok, width = normed.shape
    span = 4 * tok
    q_width, kv_width = w_query.shape[1], w_key.shape[1]
    slots = group_count if exchange else 1
    hbm = pl.BlockSpec(memory_space=pl.ANY)
    return pl.pallas_call(
        functools.partial(project_kernel, exchange),
        out_shape=(
            jax.ShapeDtypeStruct((span, q_width), jnp.bfloat16),
            jax.ShapeDtypeStruct((slots, span, 2 * kv_width), jnp.bfloat16),
        ),
        in_specs=[VMEM_SPEC, hbm, hbm, hbm, VMEM_SPEC, VMEM_SPEC],
        out_specs=(VMEM_SPEC, VMEM_SPEC),
        scratch_shapes=[
            pltpu.VMEM((span, width), jnp.bfloat16),
            pltpu.VMEM(w_query.shape, jnp.bfloat16),
            pltpu.VMEM(w_key.shape, jnp.bfloat16),
            pltpu.VMEM(w_value.shape, jnp.bfloat16),
            pltpu.SemaphoreType.DMA((2,)),
            pltpu.SemaphoreType.DMA((4,)),
            pltpu.SemaphoreType.DMA((4,)),
            pltpu.SemaphoreType.DMA((3,)),
            pltpu.SemaphoreType.DMA((4, 9)),
            pltpu.SemaphoreType.DMA((4, 9)),
        ],
        compiler_params=pltpu.CompilerParams(
            collective_id=0, has_side_effects=True, vmem_limit_bytes=VMEM_BYTES
        ),
        name="project",
    )(normed, w_query, w_key, w_value, cosine, sine)


def attend_kernel(
    key_rows, q_rows, bounds_ref, q_ref, kv_ref, key_place_ref, q_place_ref, q_start_ref, back_ref,
    out_ref, context,
):
    sources = kv_ref.shape[0]
    kv_count = kv_ref.shape[2] // (2 * HEAD_DIM)
    blocks, block_rows, width = q_ref.shape
    group = width // HEAD_DIM // kv_count
    piece = q_rows // blocks
    chunk = sources * key_rows
    scale = HEAD_DIM ** (-0.5) * LOG2E
    stack = group * q_rows

    def tile_step(t, _):
        at = pl.ds(pl.multiple_of(t * q_rows, q_rows), q_rows)
        place = q_place_ref[at, :]
        start = q_start_ref[at, :]
        inner = pl.ds(pl.multiple_of(t * piece, piece), piece)
        queries = []
        for h in range(kv_count):
            queries.append(
                jnp.concatenate(
                    [
                        q_ref[
                            :, inner, (h * group + j) * HEAD_DIM : (h * group + j + 1) * HEAD_DIM
                        ].reshape(q_rows, HEAD_DIM)
                        for j in range(group)
                    ],
                    axis=0,
                )
            )

        def chunk_step(b, carry):
            places = key_place_ref[b]
            bias = jnp.where(
                (places >= start) & (places <= place), jnp.float32(0), jnp.float32(score_floor)
            )
            bias = jnp.concatenate([bias] * group, axis=0)
            rows = pl.ds(pl.multiple_of(b * key_rows, key_rows), key_rows)
            after = []
            for h in range(kv_count):
                peak, total, mixed = carry[h]
                keys = kv_ref[:, rows, h * HEAD_DIM : (h + 1) * HEAD_DIM].reshape(chunk, HEAD_DIM)
                low = (kv_count + h) * HEAD_DIM
                values = kv_ref[:, rows, low : low + HEAD_DIM].reshape(chunk, HEAD_DIM)
                scores = (
                    lax.dot_general(
                        queries[h], keys, (((1,), (1,)), ((), ())),
                        preferred_element_type=jnp.float32,
                    )
                    * scale
                    + bias
                )
                new_peak = jnp.maximum(peak, jnp.max(scores, axis=1, keepdims=True))
                weights = jnp.exp2(scores - new_peak)
                fade = jnp.exp2(peak - new_peak)
                total = total * fade + jnp.sum(weights, axis=1, keepdims=True)
                mixed = mixed * fade + jnp.dot(
                    weights.astype(jnp.bfloat16), values, preferred_element_type=jnp.float32
                )
                after.append((new_peak, total, mixed))
            return tuple(after)

        first = tuple(
            (
                jnp.full((stack, 1), score_floor, jnp.float32),
                jnp.zeros((stack, 1), jnp.float32),
                jnp.zeros((stack, HEAD_DIM), jnp.float32),
            )
            for _ in range(kv_count)
        )
        last = lax.fori_loop(bounds_ref[0, t], bounds_ref[1, t], chunk_step, first)
        for h in range(kv_count):
            _, total, mixed = last[h]
            done = (mixed / total).astype(jnp.bfloat16)
            for j in range(group):
                head = (h * group + j) * HEAD_DIM
                context[:, inner, head : head + HEAD_DIM] = done[
                    j * q_rows : (j + 1) * q_rows
                ].reshape(blocks, piece, HEAD_DIM)
        return 0

    lax.fori_loop(0, block_rows // piece, tile_step, 0)

    for j in range(blocks):
        out_ref[j] = jnp.dot(
            back_ref[j], context[j], preferred_element_type=jnp.float32
        ).astype(jnp.bfloat16)


def attend(bounds, query, kv_all, key_place, q_place, q_start, back, key_rows, q_rows):
    return pl.pallas_call(
        functools.partial(attend_kernel, key_rows, q_rows),
        out_shape=jax.ShapeDtypeStruct(query.shape, jnp.bfloat16),
        in_specs=[pl.BlockSpec(memory_space=pltpu.SMEM)] + [VMEM_SPEC] * 6,
        out_specs=VMEM_SPEC,
        scratch_shapes=[pltpu.VMEM(query.shape, jnp.bfloat16)],
        compiler_params=pltpu.CompilerParams(vmem_limit_bytes=VMEM_BYTES),
        name="attend",
    )(bounds, query, kv_all, key_place, q_place, q_start, back)


def output_kernel(
    context_ref, w_ref, tokens_ref, out_ref,
    far_out, right_out, left_out, relay, from_left, from_right, send_sem, recv_sem,
):
    tok, width = tokens_ref.shape
    half = width // 2
    dp = lax.axis_index("dp")
    me = lax.axis_index("tp")
    right, left = lax.rem(me + 1, 4), lax.rem(me + 3, 4)
    far = lax.rem(me + 2, 4)
    go_right, go_left = (dp, right), (dp, left)
    greet([go_right, go_left])
    columns = (pl.ds(0, half), pl.ds(half, half))
    tile = 256

    def fill(owner, dst, side, more=None):
        rows = pl.ds(pl.multiple_of(owner * tok, tok), tok)

        def step(i, _):
            at = pl.ds(pl.multiple_of(side * half + i * tile, tile), tile)
            term = jnp.dot(context_ref[rows, :], w_ref[:, at], preferred_element_type=jnp.float32)
            if more is not None:
                part = pl.ds(pl.multiple_of(i * tile, tile), tile)
                term = term + more[:, part].astype(jnp.float32)
            at_half = pl.ds(pl.multiple_of(i * tile, tile), tile)
            dst[side, :, at_half] = term.astype(jnp.bfloat16)
            return 0

        lax.fori_loop(0, half // tile, step, 0)

    def put(src, dst, i, where):
        copy = remote(src, dst, send_sem.at[i], recv_sem.at[i], where)
        copy.start()
        return copy

    fill(far, far_out, 0)
    far_right = put(far_out.at[0], relay.at[0], 0, go_right)
    fill(far, far_out, 1)
    far_left = put(far_out.at[1], relay.at[1], 1, go_left)
    fill(right, right_out, 1)
    near_right = put(right_out.at[1], from_left.at[1], 2, go_right)
    fill(left, left_out, 0)
    near_left = put(left_out.at[0], from_right.at[0], 3, go_left)
    far_right.wait_recv()
    fill(right, right_out, 0, relay.at[0])
    sum_right = put(right_out.at[0], from_left.at[0], 4, go_right)
    far_left.wait_recv()
    fill(left, left_out, 1, relay.at[1])
    sum_left = put(left_out.at[1], from_right.at[1], 5, go_left)
    near_right.wait_recv()
    near_left.wait_recv()

    rows = pl.ds(pl.multiple_of(me * tok, tok), tok)
    sums = (sum_right, sum_left)
    for copy in sums:
        copy.wait_recv()
    for side in range(2):

        def last_step(i, _):
            at = pl.ds(pl.multiple_of(side * half + i * tile, tile), tile)
            part = pl.ds(pl.multiple_of(i * tile, tile), tile)
            term = jnp.dot(context_ref[rows, :], w_ref[:, at], preferred_element_type=jnp.float32)
            term = term + from_left[side, :, part].astype(jnp.float32)
            term = term + from_right[side, :, part].astype(jnp.float32)
            out_ref[:, at] = (term + tokens_ref[:, at].astype(jnp.float32)).astype(jnp.bfloat16)
            return 0

        lax.fori_loop(0, half // tile, last_step, 0)
    for copy in (far_right, far_left, near_right, near_left, sum_right, sum_left):
        copy.wait_send()


def project_out(context, w_output, tokens):
    tok, width = tokens.shape
    pair = pltpu.VMEM((2, tok, width // 2), jnp.bfloat16)
    return pl.pallas_call(
        output_kernel,
        out_shape=jax.ShapeDtypeStruct(tokens.shape, jnp.bfloat16),
        in_specs=[VMEM_SPEC] * 3,
        out_specs=VMEM_SPEC,
        scratch_shapes=[pair] * 6
        + [pltpu.SemaphoreType.DMA((6,)), pltpu.SemaphoreType.DMA((6,))],
        compiler_params=pltpu.CompilerParams(
            collective_id=1, has_side_effects=True, vmem_limit_bytes=VMEM_BYTES
        ),
        name="project_out",
    )(context, w_output, tokens)


def body(tokens, norm_gain, w_query, w_key, w_value, w_output, doc_lengths, pack_index):
    group_count = lax.axis_size("dp")
    tp_count = lax.axis_size("tp")
    tok_dev = tokens.shape[0]
    span = tp_count * tok_dev
    my_group = lax.axis_index("dp")
    exchange = group_count == 8
    q_rows = 64
    source_count = group_count * tp_count
    key_rows = max(16, 512 // source_count)
    key_chunks = tok_dev // key_rows

    packs = pack_index.reshape(source_count, tok_dev)
    order = jnp.arange(tok_dev, dtype=jnp.int32)
    rank = jnp.sum((packs[:, None, :] < packs[:, :, None]).astype(jnp.int32), axis=2)
    sorted_packs = jnp.sum(
        jnp.where(rank[:, None, :] == order[None, :, None], packs[:, None, :], 0), axis=2
    )
    key_place = (
        sorted_packs.reshape(source_count, key_chunks, key_rows)
        .transpose(1, 0, 2)
        .reshape(key_chunks, 1, source_count * key_rows)
    )
    chunk_low = jnp.min(key_place, axis=(1, 2))
    chunk_high = jnp.max(key_place, axis=(1, 2))

    doc_ends = jnp.cumsum(doc_lengths)
    doc_starts = doc_ends - doc_lengths

    def start_of(place):
        inside = (place[:, None] >= doc_starts[None, :]) & (place[:, None] < doc_ends[None, :])
        return jnp.sum(jnp.where(inside, doc_starts[None, :], 0), axis=1)

    my_rank = lax.dynamic_slice_in_dim(rank, my_group * tp_count, tp_count)
    my_sorted = lax.dynamic_slice_in_dim(sorted_packs, my_group * tp_count, tp_count)
    own_rank = lax.dynamic_index_in_dim(my_rank, lax.axis_index("tp"), 0, keepdims=False)
    sort = (own_rank[None, :] == order[:, None]).astype(jnp.bfloat16)
    back = (my_rank[:, :, None] == order[None, None, :]).astype(jnp.bfloat16)
    my_pack = my_sorted.reshape(span)
    my_start = start_of(my_pack)

    def by_tile(rows):
        pieces = rows.reshape(tp_count, -1, q_rows // tp_count)
        return pieces.transpose(1, 0, 2).reshape(-1, q_rows)

    q_place, q_start = by_tile(my_pack), by_tile(my_start)
    tile_low, tile_high = jnp.min(q_start, axis=1), jnp.max(q_place, axis=1)
    bounds = jnp.stack(
        [
            jnp.sum((chunk_high[None, :] < tile_low[:, None]).astype(jnp.int32), axis=1),
            jnp.sum((chunk_low[None, :] <= tile_high[:, None]).astype(jnp.int32), axis=1),
        ]
    )

    position = my_pack - my_start
    half_dim = HEAD_DIM // 2
    frequency = rope_base ** (-2.0 * jnp.arange(half_dim, dtype=jnp.float32) / HEAD_DIM)
    angles = position.astype(jnp.float32)[:, None] * frequency[None, :]
    cos_half, sin_half = jnp.cos(angles), jnp.sin(angles)
    cosine = jnp.concatenate([cos_half, cos_half], axis=1)
    sine = jnp.concatenate([-sin_half, sin_half], axis=1)

    residual = tokens.astype(jnp.float32)
    normed = (
        residual
        * lax.rsqrt(jnp.mean(residual * residual, axis=1, keepdims=True) + norm_eps)
        * norm_gain
    ).astype(jnp.bfloat16)
    normed = jnp.dot(sort, normed, preferred_element_type=jnp.float32).astype(jnp.bfloat16)
    query, kv = project(normed, w_query, w_key, w_value, cosine, sine, exchange, group_count)
    if not exchange:
        kv = lax.all_gather(kv[0], "dp", axis=0)
    context = attend(
        bounds,
        query.reshape(tp_count, tok_dev, -1),
        kv.reshape(source_count, tok_dev, -1),
        key_place,
        q_place.reshape(span, 1),
        q_start.reshape(span, 1),
        back,
        key_rows,
        q_rows,
    )
    return project_out(context.reshape(span, -1), w_output, tokens)


def solution(mesh):
    placed = (
        P(("dp", "tp"), None),
        P(),
        P(None, "tp"),
        P(None, "tp"),
        P(None, "tp"),
        P("tp", None),
        P(),
        P(),
    )
    return jax.shard_map(
        body, mesh=mesh, in_specs=placed, out_specs=P(("dp", "tp"), None), check_vma=False
    )
```
